32 devices in a mesh: band: 4 (over y, x), chan: 8 (over z, core).
Axes of the slice: x: 2, y: 2, z: 4, core: 2. Of those that a mesh axis runs over, the one named last changes fastest.
Arguments:
- coeffs: bfloat16 [2, 8, 1024, 4096], P(None, None, 'chan', 'band'), may hold values from -1100 to 1100, as said below
Outputs:
- coherence: float32 [1024, 1024], P('chan', 'band')
The draws below stay inside these ranges and needn't reach their ends.
Inputs may be any that keep to these rules, and one draw needn't show every extreme that they name: `coeffs`: finite real and imaginary parts.
All inputs are finite; a program needn't handle non-finite values.
Results may differ from the reference program's by a relative error of at most 0.0003.
Values may be sent and summed in bfloat16 or wider, within the bound.
A program may use at most 192 MiB of HBM per device.

```python
import jax
import jax.numpy as jnp
from jax import lax

C = 1024
K = 8
W = 16
BINS = 4096


def draw_coeffs(key, part):
    noise_key = jax.random.fold_in(jax.random.fold_in(key, 17), 0)
    noise = jnp.clip(jax.random.normal(noise_key, (2, K, C, BINS), jnp.float32), -6.0, 6.0)
    values = noise
    return values.astype(jnp.bfloat16)


def setup_inputs(seed: int = 0) -> dict:
    splits = jax.random.split(jax.random.key(seed), 2)
    return {
        "coeffs": draw_coeffs(jax.random.fold_in(splits[1], 71), 0),
    }


epsilon = 1e-6


def band_term(total, block):
    width = block.shape[2]
    flat = block.transpose(2, 0, 1, 3).reshape(width, -1)
    paired = jnp.stack((block[1], -block[0]), axis=0).transpose(2, 0, 1, 3).reshape(width, -1)
    real_part = jnp.dot(flat, flat.T, preferred_element_type=jnp.float32)
    imag_part = jnp.dot(paired, flat.T, preferred_element_type=jnp.float32)
    wide = flat.astype(jnp.float32)
    power = jnp.sum(wide * wide, axis=1) + epsilon
    coh_band = (real_part * real_part + imag_part * imag_part) / (power[:, None] * power[None, :])
    return total + coh_band, None


def reference(coeffs):
    num_bands = BINS // W
    width = coeffs.shape[2]
    blocks = coeffs.reshape(2, K, width, num_bands, W)
    blocks = jnp.moveaxis(blocks, 3, 0)
    total, unused = lax.scan(band_term, jnp.zeros((width, width), jnp.float32), blocks)
    rows = lax.broadcasted_iota(jnp.int32, (width, width), 0)
    cols = lax.broadcasted_iota(jnp.int32, (width, width), 1)
    total = jnp.where(rows == cols, jnp.float32(0.0), total)
    return total * jnp.float32(W * K / num_bands)
```

```python
import functools

import jax
import jax.numpy as jnp
from jax import lax
from jax.experimental import pallas as pl
from jax.experimental.pallas import tpu as pltpu
from jax.sharding import PartitionSpec as P

W = 16

epsilon = 1e-06

MESH = pl.DeviceIdType.MESH


def partner(index, size, offset):
    other = index
    bit = 1
    while bit < size:
        if offset & bit:
            other = other + (1 - 2 * ((index // bit) % 2)) * bit
        bit *= 2
    return other


def kernel(x_ref, out_ref, buf, sel, xb, xq, inv_col, inv_row, own_sem, send_sem, recv_sem):
    n = lax.axis_size("chan")
    me = lax.axis_index("chan")
    parts, tapers, own, wide = buf.shape[1:]
    bands, full, depth = xb.shape
    lanes = bands * W
    half = depth // 2
    tile = min(256, full)

    def window(device):
        return pl.ds(pl.multiple_of(device * lanes // wide * wide, wide), wide)

    barrier = pltpu.get_barrier_semaphore()
    for offset in range(1, n):
        pl.semaphore_signal(
            barrier, inc=1, device_id={"chan": partner(me, n, offset)}, device_id_type=MESH
        )

    local = pltpu.make_async_copy(
        x_ref.at[:, :, :, window(me)], buf.at[me], own_sem
    )
    local.start()
    pl.semaphore_wait(barrier, n - 1)

    copies = {}
    for offset in reversed(range(1, n)):
        peer = partner(me, n, offset)
        copies[offset] = pltpu.make_async_remote_copy(
            src_ref=x_ref.at[:, :, :, window(peer)],
            dst_ref=buf.at[me],
            send_sem=send_sem.at[offset],
            recv_sem=recv_sem.at[offset],
            device_id={"chan": peer},
            device_id_type=MESH,
        )
        copies[offset].start()

    row = lax.broadcasted_iota(jnp.int32, (wide, bands * half), 0) - (me * lanes) % wide
    col = lax.broadcasted_iota(jnp.int32, (wide, bands * half), 1)
    band, within = col // half, col % half
    for k in range(tapers):
        hit = (row == band * W + within - k * W) & (within // W == k)
        sel[k * wide : (k + 1) * wide, :] = jnp.where(hit, 1.0, 0.0).astype(jnp.bfloat16)

    def relayout(src):
        rows = pl.ds(pl.multiple_of(src * own, own), own)
        re = jnp.concatenate([buf[src, 0, k] for k in range(tapers)], axis=1)
        im = jnp.concatenate([buf[src, 1, k] for k in range(tapers)], axis=1)
        lane = lax.broadcasted_iota(jnp.int32, (own, 128), 1)
        power = jnp.ones((own, 128), jnp.float32)
        for b in range(bands):
            chosen = sel[:, b * half : (b + 1) * half]
            re_b = jnp.dot(re, chosen, preferred_element_type=jnp.float32)
            im_b = jnp.dot(im, chosen, preferred_element_type=jnp.float32)
            total = jnp.sum(re_b * re_b + im_b * im_b, axis=1, keepdims=True) + epsilon
            power = jnp.where(lane == b, total, power)
            xb[b, rows, :half] = re_b.astype(jnp.bfloat16)
            xb[b, rows, half:] = im_b.astype(jnp.bfloat16)
            xq[b, rows, :half] = im_b.astype(jnp.bfloat16)
            xq[b, rows, half:] = (-re_b).astype(jnp.bfloat16)
        inv_col[rows, :] = 1.0 / power

    local.wait()
    relayout(me)
    for offset in range(1, n):
        copies[offset].wait_recv()
        relayout(partner(me, n, offset))

    count = full // tile
    for i in range(count):
        turned = inv_col[i * tile : (i + 1) * tile, :].T
        inv_row[:, i * tile : (i + 1) * tile] = turned[:bands, :]

    contract = (((1,), (1,)), ((), ()))
    for i in range(count):
        row0 = i * tile

        def column(j, carry):
            col0 = pl.multiple_of(j * tile, tile)
            acc = jnp.zeros((tile, tile), jnp.float32)
            for b in range(bands):
                right = xb[b, pl.ds(col0, tile), :]
                re = lax.dot_general(
                    xb[b, row0 : row0 + tile, :], right, contract, preferred_element_type=jnp.float32
                )
                im = lax.dot_general(
                    xq[b, row0 : row0 + tile, :], right, contract, preferred_element_type=jnp.float32
                )
                acc += ((re * re + im * im) * inv_col[row0 : row0 + tile, b : b + 1]) * inv_row[
                    b : b + 1, pl.ds(col0, tile)
                ]
            out_ref[row0 : row0 + tile, pl.ds(col0, tile)] = acc
            out_ref[pl.ds(col0, tile), row0 : row0 + tile] = acc.T
            return carry

        lax.fori_loop(i, count, column, 0)

    for offset in range(1, n):
        copies[offset].wait_send()


def body(coeffs):
    parts, tapers, own, bins = coeffs.shape
    n = lax.axis_size("chan")
    groups = lax.axis_size("band")
    full = own * n
    lanes = bins // n
    wide = max(lanes, 128)
    bands = lanes // W
    depth = parts * tapers * W
    scale = jnp.float32(W * tapers / (bins // W * groups))
    partial_sum = pl.pallas_call(
        kernel,
        out_shape=jax.ShapeDtypeStruct((full, full), jnp.float32),
        in_specs=[pl.BlockSpec(memory_space=pl.ANY)],
        out_specs=pl.BlockSpec(memory_space=pltpu.VMEM),
        scratch_shapes=[
            pltpu.VMEM((n, parts, tapers, own, wide), jnp.bfloat16),
            pltpu.VMEM((tapers * wide, bands * tapers * W), jnp.bfloat16),
            pltpu.VMEM((bands, full, depth), jnp.bfloat16),
            pltpu.VMEM((bands, full, depth), jnp.bfloat16),
            pltpu.VMEM((full, 128), jnp.float32),
            pltpu.VMEM((bands, full), jnp.float32),
            pltpu.SemaphoreType.DMA,
            pltpu.SemaphoreType.DMA((n,)),
            pltpu.SemaphoreType.DMA((n,)),
        ],
        compiler_params=pltpu.CompilerParams(
            collective_id=0, has_side_effects=True, vmem_limit_bytes=48 * 1024 * 1024
        ),
    )(coeffs)
    summed = lax.psum_scatter(partial_sum, "band", scatter_dimension=1, tiled=True)
    summed = lax.psum_scatter(summed, "chan", scatter_dimension=0, tiled=True)
    share = full // groups
    row_global = lax.broadcasted_iota(jnp.int32, (own, share), 0) + lax.axis_index("chan") * own
    col_global = lax.broadcasted_iota(jnp.int32, (own, share), 1) + lax.axis_index("band") * share
    return jnp.where(row_global == col_global, jnp.float32(0.0), summed) * scale


def solution(mesh):
    return jax.shard_map(
        body,
        mesh=mesh,
        in_specs=(P(None, None, "chan", "band"),),
        out_specs=P("chan", "band"),
        check_vma=False,
    )
```
